32 devices in a mesh: dp: 4 (over y, x), space: 8 (over z, core).
Axes of the slice: x: 2, y: 2, z: 4, core: 2. Of those that a mesh axis runs over, the one named last changes fastest.
Arguments:
- fields: bfloat16 [4, 100, 32768], P('dp', None, 'space'), may hold values from -6 to 6
- cell_index: int32 [256, 128], P('space'), may hold values from 0 to 6143
- interp_weight: bfloat16 [256, 16, 128], P('space'), may hold values from 0 to 2, as said below
- w_in: bfloat16 [100, 1024], replicated, may hold values from -0.625 to 0.625
- ln_gain: float32 [1024], replicated, may hold values from 0.5 to 1.5
- w_qkv: bfloat16 [1024, 3072], P('dp'), may hold values from -0.1875 to 0.1875
- w_out: bfloat16 [1024, 1024], P('dp'), may hold values from -3 to 3
Outputs:
- latent: bfloat16 [4, 4096, 1024], P('dp', 'space')
- update: bfloat16 [4, 4096, 1024], P('dp', 'space')
The draws below stay inside these ranges and needn't reach their ends.
Inputs may be any that keep to these rules, and one draw needn't show every extreme that they name: `interp_weight`: in each block the slots from some count on carry zero weight for all its 16 nodes; that count lies between 48 and 128. `cell_index`: indexes a shard's 4096 cells extended by 1024 cells of each neighbouring shard, lower neighbour first.
All inputs are finite; a program needn't handle non-finite values.
Results may differ from the reference program's by a relative error of at most 0.0068.
Values may be sent and summed in bfloat16 or wider, within the bound.
A program may use at most 128 MiB of HBM per device.

```python
import math
import jax
import jax.numpy as jnp
from jax import lax

D = 1024
HEADS = 16
CH = 100
NBLK = 16
SLOTS = 128
NODE_DEV = 512
CELL_DEV = 4096
HEAD_SIZE = 64
HALO_C = 1024
HALO_N = 256
BLK_DEV = 32
SAMPLES = 4
NODES = 4096
CELLS = 32768
BLOCKS = 256
N_SPACE = 8


def draw_interp_weight(key, part):
    count_key, chosen_key, magnitude_key = jax.random.split(key, 3)
    full_shape = (BLOCKS, NBLK, SLOTS)
    live_count = jax.random.randint(count_key, (BLOCKS, 1, 1), 3 * SLOTS // 8, SLOTS + 1)
    slot_index = lax.broadcasted_iota(jnp.int32, full_shape, 2)
    chosen = jax.random.randint(chosen_key, full_shape, 0, 2)
    kept_mask = (slot_index < live_count) & (chosen == 0)
    magnitude = jax.random.uniform(magnitude_key, full_shape, jnp.float32, 0.0, 1.0)
    return jnp.where(kept_mask, magnitude, 0.0).astype(jnp.float32).astype(jnp.bfloat16)


def plant(array, rng, low, largest):
    spot = [jax.random.randint(jax.random.fold_in(rng, axis), (), 0, length) for axis, length in enumerate(array.shape)]
    longest = array.shape.index(max(array.shape))
    beside = spot[:longest] + [(spot[longest] + 1) % array.shape[longest]] + spot[longest + 1:]
    return array.at[tuple(spot)].set(low).at[tuple(beside)].set(largest)


def block_scale(stream_key, dims, shards, least, top_value):
    level, own = 1.0, jax.random.fold_in(stream_key, 6)
    for axis_at, shards_of in shards:
        heights = jnp.exp(jax.random.uniform(jax.random.fold_in(own, axis_at), (shards_of,), jnp.float32, least / len(shards), top_value / len(shards)))
        level = level * jnp.repeat(heights, dims[axis_at] // shards_of).reshape([-1 if axis == axis_at else 1 for axis in range(len(dims))])
    return level


def bell_draw(key, extent, width, bound, shards=(), kind=jnp.bfloat16):
    entries = width * jax.random.normal(key, extent, jnp.float32)
    if shards:
        entries = entries * block_scale(key, extent, shards, -0.22, 0.18)
    return jnp.clip(entries, -bound, bound).astype(kind)


def setup_inputs(seed: int = 0) -> dict:
    seeds = jax.random.split(jax.random.key(seed), 8)
    fields = bell_draw(seeds[0], (SAMPLES, CH, CELLS), 1.0, 6.0, ((0, 4), (2, 8)))
    cell_index = plant(jax.random.randint(seeds[1], (BLOCKS, SLOTS), 0, CELL_DEV + 2 * HALO_C), jax.random.fold_in(seeds[1], 1), 0, (CELL_DEV + 2 * HALO_C) - 1).astype(jnp.int32)
    interp_weight = draw_interp_weight(jax.random.fold_in(seeds[7], 71), 0)
    w_in = bell_draw(seeds[3], (CH, D), CH ** -0.5, 0.625)
    ln_gain = jnp.clip(1.0 + 0.1 * jax.random.normal(seeds[4], (D,), jnp.float32), 0.5, 1.5)
    w_qkv = bell_draw(seeds[5], (D, 3 * D), D ** -0.5, 0.1875, ((0, 4),))
    w_out = bell_draw(seeds[6], (D, D), (max(D // 256, 1)) ** -0.5, 3.0, ((0, 4),))
    return {"fields": fields, "cell_index": cell_index, "interp_weight": interp_weight, "w_in": w_in, "ln_gain": ln_gain, "w_qkv": w_qkv, "w_out": w_out}


def unit_heads(projected):
    head_rows = projected.reshape(projected.shape[0], HEADS, HEAD_SIZE)
    scale_rows = jnp.sqrt(lax.optimization_barrier(jnp.mean(head_rows * head_rows, axis=-1, keepdims=True)) + 1e-06)
    return (head_rows / scale_rows).astype(jnp.bfloat16)

def one_sample(grid_field, cell_index, interp_weight, w_in, ln_gain, w_qkv, w_out):
    owner_shard = jnp.arange(BLOCKS, dtype=jnp.int32) // BLK_DEV
    source = (owner_shard[:, None] * CELL_DEV - HALO_C + cell_index) % CELLS
    picked = jnp.take(grid_field, source.astype(jnp.int32), axis=1).astype(jnp.float32)
    encoded = jnp.einsum('cbs,bns->bnc', picked, interp_weight.astype(jnp.float32))
    encoded = encoded.reshape(NODES, CH).astype(jnp.bfloat16)
    embedded = jnp.dot(encoded, w_in, preferred_element_type=jnp.float32)
    average = lax.optimization_barrier(jnp.mean(embedded, axis=1, keepdims=True))
    centered = embedded - average
    spread = lax.optimization_barrier(jnp.mean(centered * centered, axis=1, keepdims=True))
    normed = (centered / jnp.sqrt(spread + 1e-05) * ln_gain).astype(jnp.bfloat16)
    projected = jnp.dot(normed, w_qkv, preferred_element_type=jnp.float32)
    queries = unit_heads(projected[:, :D])
    keys_all = unit_heads(projected[:, D:2 * D])
    values_all = projected[:, 2 * D:].reshape(NODES, HEADS, HEAD_SIZE).astype(jnp.bfloat16)
    wrapped_keys = jnp.concatenate([keys_all[NODES - HALO_N:], keys_all, keys_all[:HALO_N]], axis=0)
    wrapped_values = jnp.concatenate([values_all[NODES - HALO_N:], values_all, values_all[:HALO_N]], axis=0)

    def attend(shard_index):
        first_row = shard_index * NODE_DEV
        query_rows = lax.dynamic_slice_in_dim(queries, first_row, NODE_DEV, 0).astype(jnp.float32)
        key_rows = lax.dynamic_slice_in_dim(wrapped_keys, first_row, NODE_DEV + 2 * HALO_N, 0).astype(jnp.float32)
        value_rows = lax.dynamic_slice_in_dim(wrapped_values, first_row, NODE_DEV + 2 * HALO_N, 0).astype(jnp.float32)
        scores = jnp.einsum('qhd,khd->hqk', query_rows, key_rows) / math.sqrt(HEAD_SIZE)
        weights = jnp.exp(scores)
        probs = (weights / lax.optimization_barrier(jnp.sum(weights, axis=2, keepdims=True))).astype(jnp.bfloat16)
        mixed_rows = jnp.einsum('hqk,khd->qhd', probs.astype(jnp.float32), value_rows)
        return mixed_rows.astype(jnp.bfloat16).reshape(NODE_DEV, D)
    attended = lax.map(attend, jnp.arange(N_SPACE, dtype=jnp.int32)).reshape(NODES, D)
    update = jnp.dot(attended, w_out, preferred_element_type=jnp.float32).astype(jnp.bfloat16)
    return (embedded.astype(jnp.bfloat16), update)

def reference(fields, cell_index, interp_weight, w_in, ln_gain, w_qkv, w_out):

    def per_sample(grid_field):
        return one_sample(grid_field, cell_index, interp_weight, w_in, ln_gain, w_qkv, w_out)
    latent, update = lax.map(per_sample, fields)
    return (latent, update)
```

```python
import functools

import jax
import jax.numpy as jnp
from jax import lax
from jax.experimental import pallas as pl
from jax.experimental.pallas import tpu as pltpu
from jax.sharding import PartitionSpec as P

HEADS = 16
GROUP_HEADS = 4
F32, BF16 = jnp.float32, jnp.bfloat16
MESH = pl.DeviceIdType.MESH
CONTRACT_LAST = (((1,), (1,)), ((), ()))


def kernel(
    n, space, index_hbm, field_hbm, weight_hbm, w_in_hbm, gain_hbm, w_qkv_hbm, w_out_hbm,
    att_ref, wo_ref, enc_out, w_in_full,
    index_ref, field_ref, weight_ref, w_in_ref, gain_ref,
    low_ref, high_ref, cells_ref, picked_ref, enc_ref, normed_ref, wq_ref,
    q_ref, k_ref, vt_ref,
    in_sem, local_sem, field_send, field_recv, enc_send, enc_recv, norm_send, norm_recv,
    a_send, a_recv, z_send, z_recv, swap_send, swap_recv, give_send, give_recv,
):
    d, s = lax.axis_index("dp"), lax.axis_index("space")
    up, down = lax.rem(s + 1, space), lax.rem(s + space - 1, space)
    core = lax.rem(s, 2)
    partner = s + 1 - 2 * core
    outer = lax.rem(s + space - 1 + 2 * core, space)
    layer = lax.rem(s // 2, 2)
    beside = s + 2 - 4 * layer
    share = n == 4 and space % 4 == 0
    channels, cell_count = field_ref.shape
    reach = low_ref.shape[1]
    rows, width = w_out_hbm.shape
    gw = q_ref.shape[1]
    parts = width // gw
    groups = parts // 2
    chunks = 3 * groups + parts // 2
    head_size = gw // GROUP_HEADS
    nodes = enc_out.shape[0]
    margin = nodes // 2
    side = nodes + margin
    window = nodes + 2 * margin
    blocks, per_block, slots = weight_ref.shape
    if n == 4:
        peers = [d + 1 - 2 * lax.rem(d, 2), lax.rem(d + 2, 4), 3 - d]
    else:
        peers = [lax.rem(d + i, n) for i in range(1, n)]

    def source_of(i):
        return peers[i] if n == 4 else peers[n - 2 - i]

    barrier = pltpu.get_barrier_semaphore()
    for peer in peers:
        pl.semaphore_signal(barrier, inc=1, device_id=(peer, s), device_id_type=MESH)
    near = (up, down, beside) if share else (up, down)
    for peer in near:
        pl.semaphore_signal(barrier, inc=1, device_id=(d, peer), device_id_type=MESH)

    inputs = [
        pltpu.make_async_copy(source, target, in_sem.at[i])
        for i, (source, target) in enumerate((
            (field_hbm, field_ref), (index_hbm, index_ref), (weight_hbm, weight_ref),
            (w_in_hbm, w_in_ref), (gain_hbm, gain_ref)))
    ]
    for copy in inputs:
        copy.start()

    def chunk(c):
        return wq_ref.at[c] if c < 3 * groups else wo_ref.at[groups * core + c - 3 * groups]

    own = pl.ds(pl.multiple_of(d * rows, rows), rows)
    order = [3 * g + t for g in range(groups) for t in (1, 0, 2)]
    order += range(3 * groups, chunks)
    local = {}
    for c in order:
        if c < 3 * groups:
            column = c % 3 * width + (core * groups + c // 3) * gw
            source = w_qkv_hbm.at[:, pl.ds(pl.multiple_of(column, gw), gw)]
        else:
            column = (core * groups + c - 3 * groups) * gw
            source = w_out_hbm.at[:, pl.ds(pl.multiple_of(column, gw), gw)]
        local[c] = pltpu.make_async_copy(source, chunk(c).at[own, :], local_sem.at[c])
        local[c].start()

    def remote(src, dst, send, recv, device):
        return pltpu.make_async_remote_copy(
            src_ref=src, dst_ref=dst, send_sem=send, recv_sem=recv,
            device_id=device, device_id_type=MESH)

    field_up = remote(field_ref.at[:, pl.ds(cell_count - reach, reach)], low_ref,
                      field_send.at[0], field_recv.at[0], (d, up))
    field_down = remote(field_ref.at[:, pl.ds(0, reach)], high_ref,
                        field_send.at[1], field_recv.at[1], (d, down))

    whole = rows * 11 // 256 * 16
    half = rows // 2

    def span(c, i, mine):
        if not share:
            return 0, rows
        at = layer if mine else 1 - layer
        if i == 2:
            return at * half, half
        return at * (rows - whole), whole

    def passed(c, i, mine):
        at = layer if mine else 1 - layer
        if i == 2:
            return at * half, half
        return at * whole, rows - whole

    def block(c, owner, lo, size):
        return chunk(c).at[pl.ds(pl.multiple_of(owner * rows + lo, 16), size), :]

    def direct(c, i, owner):
        ref = block(c, owner, *span(c, i, True))
        return remote(ref, ref, a_send.at[c, i], a_recv.at[c, i], (peers[i], s))

    def onward(c, i, mine):
        ref = block(c, source_of(i), *passed(c, i, mine))
        return remote(ref, ref, z_send.at[c, i], z_recv.at[c, i], (d, beside))

    def begin(c):
        local[c].wait()
        for i in range(n - 1):
            direct(c, i, d).start()

    def relay(c):
        if share:
            for i in range(n - 1):
                direct(c, i, source_of(i)).wait_recv()
                onward(c, i, True).start()

    def finish(c):
        for i in range(n - 1):
            if share:
                onward(c, i, False).wait_recv()
            else:
                direct(c, i, source_of(i)).wait_recv()

    def swap(j):
        ref = wo_ref.at[j]
        at = lax.rem(j, groups)
        return remote(ref, ref, swap_send.at[at], swap_recv.at[at], (d, partner))

    pl.semaphore_wait(barrier, len(peers) + len(near))
    inputs[0].wait()
    field_up.start()
    field_down.start()
    for c in order:
        begin(c)

    unit = (lax.broadcasted_iota(jnp.int32, (channels, 128), 0)
            == lax.broadcasted_iota(jnp.int32, (channels, 128), 1)).astype(BF16)

    def turn(source, start, target):
        cells_ref[pl.ds(target, 512), :] = lax.dot_general(
            source[:, pl.ds(start, 512)], unit, (((0,), (0,)), ((), ())),
            preferred_element_type=F32)

    @pl.loop(0, cell_count // 512, unroll=2)
    def _(i):
        turn(field_ref, pl.multiple_of(i * 512, 512), pl.multiple_of(reach + i * 512, 512))

    for copy in inputs[1:]:
        copy.wait()
    pad = w_in_full.shape[0]
    w_in_full[pl.ds(pad - 32, 32), :] = jnp.zeros((32, width), BF16)
    w_in_full[pl.ds(0, channels), :] = w_in_ref[...]

    field_up.wait_recv()
    field_down.wait_recv()

    @pl.loop(0, reach // 512)
    def _(i):
        turn(low_ref, pl.multiple_of(i * 512, 512), pl.multiple_of(i * 512, 512))
        turn(high_ref, pl.multiple_of(i * 512, 512),
             pl.multiple_of(reach + cell_count + i * 512, 512))

    def gather(first, last):
        @pl.loop(first, last)
        def _(b):
            base = pl.multiple_of(b * slots, slots)
            for j in range(slots):
                picked_ref[pl.ds(base + j, 1), :] = cells_ref[pl.ds(index_ref[b, j], 1), :]

    gather(0, blocks // 2)
    relay(order[0])
    gather(blocks // 2, blocks)
    relay(order[1])

    own_base = margin + core * nodes
    own_edge = core * (nodes + margin)
    far_edge = (1 - core) * (nodes + margin)
    own_halo = core * (margin + 2 * nodes)
    far_halo = (1 - core) * (margin + 2 * nodes)
    far_base = margin + (1 - core) * nodes
    per_step = 8

    @pl.loop(0, blocks // per_step)
    def _(i):
        for j in range(per_step):
            b = i * per_step + j
            rows_b = picked_ref[pl.ds(pl.multiple_of(b * slots, slots), slots), :].astype(BF16)
            encoded = jnp.dot(weight_ref[b], rows_b, preferred_element_type=F32).astype(BF16)
            start = pl.multiple_of(b * per_block, per_block)
            enc_out[pl.ds(start, per_block), :] = encoded
            enc_ref[pl.ds(pl.multiple_of(own_base + start, per_block), per_block), :] = encoded

    def enc_copy(target):
        edge = pl.multiple_of(margin + own_edge, margin)
        return remote(enc_ref.at[pl.ds(edge, margin), :],
                      enc_ref.at[pl.ds(pl.multiple_of(target, margin), margin), :],
                      enc_send.at[0], enc_recv.at[0], (d, outer))

    enc_copy(far_halo).start()

    def embed(start):
        embedded = jnp.dot(enc_ref[pl.ds(start, 128), :], w_in_full[...], preferred_element_type=F32)
        average = jnp.mean(embedded, axis=1, keepdims=True)
        centered = embedded - average
        spread = jnp.mean(centered * centered, axis=1, keepdims=True)
        normed_ref[pl.ds(start, 128), :] = (
            centered * lax.rsqrt(spread + 1e-05) * gain_ref[...]).astype(BF16)

    def norm_copy(i, start, size):
        ref = normed_ref.at[pl.ds(pl.multiple_of(start, margin), size), :]
        return remote(ref, ref, norm_send.at[i], norm_recv.at[i], (d, partner))

    @pl.loop(0, nodes // 128, unroll=2)
    def _(i):
        embed(pl.multiple_of(own_base + i * 128, 128))

    norm_copy(0, own_base, nodes).start()
    relay(order[2])
    enc_copy(own_halo).wait_recv()

    @pl.loop(0, margin // 128, unroll=2)
    def _(i):
        embed(pl.multiple_of(own_halo + i * 128, 128))

    norm_copy(1, own_halo, margin).start()

    same_head = (lax.broadcasted_iota(jnp.int32, (gw, gw), 0) // head_size
                 == lax.broadcasted_iota(jnp.int32, (gw, gw), 1) // head_size).astype(BF16)

    def unit_heads(values):
        total = jnp.dot((values * values).astype(BF16), same_head, preferred_element_type=F32)
        return (values * lax.rsqrt(total * (1.0 / head_size) + 1e-06)).astype(BF16)

    scale = jnp.asarray(head_size ** -0.5, BF16)

    def project_part(start, size, c):
        return jnp.dot(normed_ref[pl.ds(start, size), :], wq_ref[c], preferred_element_type=F32)

    def keys(g, start):
        start = pl.multiple_of(start, margin)
        k_ref[pl.ds(start, side), :] = unit_heads(project_part(start, side, 3 * g + 1))

    def queries(g, i):
        q_ref[pl.ds(i * nodes, nodes), :] = unit_heads(
            project_part(margin + i * nodes, nodes, 3 * g)) * scale

    def values(g, start):
        start = pl.multiple_of(start, margin)
        vt_ref[:, pl.ds(start, side)] = project_part(start, side, 3 * g + 2).astype(BF16).T

    head_of = lax.broadcasted_iota(jnp.int32, (nodes, gw), 1) // head_size

    def attend(t, slot):
        start = pl.multiple_of(t * nodes, nodes)
        asked = q_ref[pl.ds(start, nodes), :]
        seen = pl.ds(start, window)

        def score(h):
            picked = jnp.where(head_of == h, asked, jnp.zeros_like(asked))
            return lax.dot_general(k_ref[seen, :], picked, CONTRACT_LAST, preferred_element_type=F32)

        outs = []
        scores = score(0)
        for h in range(GROUP_HEADS):
            weights = jnp.exp(scores)
            if h + 1 < GROUP_HEADS:
                scores = score(h + 1)
            total = jnp.sum(weights, axis=0, keepdims=True)
            out = jnp.dot(vt_ref[pl.ds(h * head_size, head_size), seen], weights.astype(BF16),
                          preferred_element_type=F32)
            outs.append(out * (1.0 / total))
        att_ref[slot] = jnp.concatenate(outs, axis=0).astype(BF16).T

    def give(g, mine):
        at = core * groups + g if mine else (1 - core) * groups + g
        return remote(att_ref.at[parts + g], att_ref.at[at], give_send.at[g], give_recv.at[g],
                      (d, partner))

    def at_group(g, value, action):
        @pl.when(g == value)
        def _():
            action()

    @pl.loop(0, groups)
    def _(g):
        for value in range(groups):
            at_group(g, value, lambda: finish(3 * value + 1))
        keys(g, own_edge)

        @pl.when(g == 0)
        def _():
            norm_copy(0, far_base, nodes).wait_recv()
            norm_copy(1, far_halo, margin).wait_recv()

        keys(g, far_edge)
        for value in range(groups):
            at_group(g, value, lambda: finish(3 * value))
        for i in range(2):
            queries(g, i)
        at_group(g, 0, lambda: relay(order[3]))
        for value in range(groups):
            at_group(g, value, lambda: finish(3 * value + 2))
        values(g, own_edge)
        values(g, far_edge)
        at_group(g, 1, lambda: relay(order[6]))

        @pl.loop(0, 2)
        def _(i):
            t = jnp.where(i == 0, 1 - core, core)
            attend(t, jnp.where(i == 0, parts + g, core * groups + g))

            @pl.when(i == 0)
            def _():
                for value in range(groups):
                    at_group(g, value, lambda: give(value, True).start())

                at_group(g, 0, lambda: relay(order[4]))

                @pl.when(g == groups - 1)
                def _():
                    relay(order[7])
                    finish(order[6])
                    swap(groups * core).start()

            @pl.when((i == 1) & (g == 0))
            def _():
                relay(order[5])

    finish(order[7])
    swap(groups * core + 1).start()
    for g in range(groups):
        give(g, False).wait_recv()
        swap(groups * (1 - core) + g).wait_recv()
    for copy in (field_up, field_down, enc_copy(far_halo), norm_copy(0, own_base, nodes),
                 norm_copy(1, own_halo, margin)):
        copy.wait_send()
    for g in range(groups):
        give(g, True).wait_send()
        swap(groups * core + g).wait_send()
    for c in order:
        for i in range(n - 1):
            direct(c, i, d).wait_send()
            if share:
                onward(c, i, True).wait_send()


def project(enc_ref, w_in_ref, att_ref, w_out_ref, latent_hbm, update_hbm,
            latent_ref, update_ref, latent_sem, update_sem):
    parts, _, gw = w_out_ref.shape
    half = enc_ref.shape[0] // 2
    copies = []
    for i in range(2):
        span = pl.ds(i * half, half)
        latent_ref[span, :] = jnp.dot(
            enc_ref[span, :], w_in_ref[...], preferred_element_type=F32).astype(BF16)
        copies.append(pltpu.make_async_copy(
            latent_ref.at[span, :], latent_hbm.at[span, :], latent_sem.at[i]))
        copies[-1].start()
    for j in range(parts):
        update_ref[j] = sum(
            jnp.dot(att_ref[g], w_out_ref[j, pl.ds(g * gw, gw), :], preferred_element_type=F32)
            for g in range(parts)).astype(BF16)
        copies.append(pltpu.make_async_copy(
            update_ref.at[j], update_hbm.at[:, pl.ds(j * gw, gw)], update_sem.at[j]))
        copies[-1].start()
    for copy in copies:
        copy.wait()


def shards(n, space, fields, cell_index, interp_weight, w_in, ln_gain, w_qkv, w_out):
    width = w_out.shape[1]
    blocks, per_block, _ = interp_weight.shape
    nodes = blocks * per_block
    channels, cells = fields.shape[1:]
    reach = cells // 4
    gw = width // HEADS * GROUP_HEADS
    parts = width // gw
    groups = parts // 2
    chunks = 3 * groups + parts // 2
    vmem = pl.BlockSpec(memory_space=pltpu.VMEM)
    hbm = pl.BlockSpec(memory_space=pl.ANY)
    dma = pltpu.SemaphoreType.DMA
    attended, w_out_full, encoded, w_in_full = pl.pallas_call(
        functools.partial(kernel, n, space),
        out_shape=[pltpu.VMEM(shape, BF16)
                   for shape in ((parts + groups, nodes, gw), (parts, width, gw),
                                 (nodes, 128), (128, width))],
        in_specs=[hbm] * 7,
        out_specs=[vmem] * 4,
        scratch_shapes=[
            pltpu.SMEM(cell_index.shape, jnp.int32),
            pltpu.VMEM((channels, cells), BF16),
            pltpu.VMEM(interp_weight.shape, BF16),
            pltpu.VMEM(w_in.shape, BF16),
            pltpu.VMEM((1, width), F32),
            pltpu.VMEM((channels, reach), BF16),
            pltpu.VMEM((channels, reach), BF16),
            pltpu.VMEM((cells + 2 * reach, 128), F32),
            pltpu.VMEM((blocks * 128, 128), F32),
            pltpu.VMEM((3 * nodes, 128), BF16),
            pltpu.VMEM((3 * nodes, width), BF16),
            pltpu.VMEM((3 * groups, width, gw), BF16),
            pltpu.VMEM((2 * nodes, gw), BF16),
            pltpu.VMEM((3 * nodes, gw), BF16),
            pltpu.VMEM((gw, 3 * nodes), BF16),
            dma((5,)), dma((chunks,)),
            dma((2,)), dma((2,)), dma((1,)), dma((1,)), dma((2,)), dma((2,)),
            dma((chunks, n - 1)), dma((chunks, n - 1)),
            dma((chunks, 3)), dma((chunks, 3)),
            dma((groups,)), dma((groups,)), dma((groups,)), dma((groups,)),
        ],
        compiler_params=pltpu.CompilerParams(
            collective_id=0, has_side_effects=True, vmem_limit_bytes=40 * 2**20),
    )(*[pltpu.with_memory_space_constraint(array, pltpu.HBM) for array in (
        cell_index, fields[0], interp_weight, w_in, ln_gain[None], w_qkv, w_out)])

    operands = [pltpu.with_memory_space_constraint(array, pltpu.VMEM)
                for array in (encoded, w_in_full, attended, w_out_full)]
    latent, update = pl.pallas_call(
        project,
        out_shape=[jax.ShapeDtypeStruct((nodes, width), BF16)] * 2,
        in_specs=[vmem] * 4,
        out_specs=[hbm] * 2,
        scratch_shapes=[
            pltpu.VMEM((nodes, width), BF16), pltpu.VMEM((parts, nodes, gw), BF16),
            dma((2,)), dma((parts,)),
        ],
        compiler_params=pltpu.CompilerParams(vmem_limit_bytes=16 * 2**20),
    )(*operands)
    return latent[None], update[None]


def solution(mesh):
    placed = (
        P("dp", None, "space"),
        P("space", None),
        P("space", None, None),
        P(),
        P(),
        P("dp", None),
        P("dp", None),
    )
    return jax.shard_map(
        functools.partial(shards, mesh.shape["dp"], mesh.shape["space"]),
        mesh=mesh,
        in_specs=placed,
        out_specs=(P("dp", "space", None), P("dp", "space", None)),
        check_vma=False,
    )
```

```python
import functools

import jax
import jax.numpy as jnp
from jax import lax
from jax.experimental import pallas as pl
from jax.experimental.pallas import tpu as pltpu
from jax.sharding import PartitionSpec as P

HEADS = 16
GROUP_HEADS = 4
F32, BF16 = jnp.float32, jnp.bfloat16
MESH = pl.DeviceIdType.MESH
SHARED = (2, 2, 2, 2, 2, 1, 2, 0)
CONTRACT_LAST = (((1,), (1,)), ((), ()))


def kernel(
    n, space, index_hbm, field_hbm, weight_hbm, w_in_hbm, gain_hbm, w_qkv_hbm, w_out_hbm,
    latent_ref, update_ref,
    index_ref, field_ref, weight_ref, w_in_ref, gain_ref,
    low_ref, high_ref, cells_ref, picked_ref, enc_ref, w_in_full, normed_ref, wq_ref,
    q_ref, k_ref, vt_ref, att_ref, wo_ref,
    in_sem, local_sem, field_send, field_recv, enc_send, enc_recv, norm_send, norm_recv,
    a_send, a_recv, z_send, z_recv, swap_send, swap_recv, give_send, give_recv,
):
    d, s = lax.axis_index("dp"), lax.axis_index("space")
    up, down = lax.rem(s + 1, space), lax.rem(s + space - 1, space)
    core = lax.rem(s, 2)
    partner = s + 1 - 2 * core
    outer = lax.rem(s + space - 1 + 2 * core, space)
    layer = lax.rem(s // 2, 2)
    beside = s + 2 - 4 * layer
    share = n == 4 and space % 4 == 0
    channels, cell_count = field_ref.shape
    reach = low_ref.shape[1]
    rows, width = w_out_hbm.shape
    gw = q_ref.shape[1]
    parts = width // gw
    groups = parts // 2
    chunks = 3 * groups + parts // 2
    head_size = gw // GROUP_HEADS
    nodes = latent_ref.shape[0]
    margin = nodes // 2
    window = nodes + 2 * margin
    blocks, per_block, slots = weight_ref.shape
    if n == 4:
        peers = [d + 1 - 2 * lax.rem(d, 2), lax.rem(d + 2, 4), 3 - d]
    else:
        peers = [lax.rem(d + i, n) for i in range(1, n)]

    def source_of(i):
        return peers[i] if n == 4 else peers[n - 2 - i]

    barrier = pltpu.get_barrier_semaphore()
    for peer in peers:
        pl.semaphore_signal(barrier, inc=1, device_id=(peer, s), device_id_type=MESH)
    near = (up, down, beside) if share else (up, down)
    for peer in near:
        pl.semaphore_signal(barrier, inc=1, device_id=(d, peer), device_id_type=MESH)

    inputs = [
        pltpu.make_async_copy(source, target, in_sem.at[i])
        for i, (source, target) in enumerate((
            (field_hbm, field_ref), (index_hbm, index_ref), (weight_hbm, weight_ref),
            (w_in_hbm, w_in_ref), (gain_hbm, gain_ref)))
    ]
    for copy in inputs:
        copy.start()

    def chunk(c):
        return wq_ref.at[c] if c < 3 * groups else wo_ref.at[groups * core + c - 3 * groups]

    own = pl.ds(pl.multiple_of(d * rows, rows), rows)
    order = [3 * g + t for g in range(groups) for t in (1, 0, 2)]
    order += range(3 * groups, chunks)
    local = {}
    for c in order:
        if c < 3 * groups:
            column = c % 3 * width + (core * groups + c // 3) * gw
            source = w_qkv_hbm.at[:, pl.ds(pl.multiple_of(column, gw), gw)]
        else:
            column = (core * groups + c - 3 * groups) * gw
            source = w_out_hbm.at[:, pl.ds(pl.multiple_of(column, gw), gw)]
        local[c] = pltpu.make_async_copy(source, chunk(c).at[own, :], local_sem.at[c])
        local[c].start()

    def remote(src, dst, send, recv, device):
        return pltpu.make_async_remote_copy(
            src_ref=src, dst_ref=dst, send_sem=send, recv_sem=recv,
            device_id=device, device_id_type=MESH)

    field_up = remote(field_ref.at[:, pl.ds(cell_count - reach, reach)], low_ref,
                      field_send.at[0], field_recv.at[0], (d, up))
    field_down = remote(field_ref.at[:, pl.ds(0, reach)], high_ref,
                        field_send.at[1], field_recv.at[1], (d, down))

    whole = rows * 11 // 256 * 16
    half = rows // 2

    level = {c: SHARED[at] if share else 0 for at, c in enumerate(order)}

    def span(c, i):
        if i == 2 and level[c]:
            return layer * half, half
        if level[c] == 2:
            return layer * (rows - whole), whole
        return 0, rows

    def passed(c, i):
        if i == 2 and level[c]:
            return layer * half, half
        return layer * whole, rows - whole

    def relayed(c):
        return [(), (2,), (0, 1, 2)][level[c]]

    def block(c, owner, lo, size):
        return chunk(c).at[pl.ds(pl.multiple_of(owner * rows + lo, 16), size), :]

    def direct(c, i):
        ref = block(c, d, *span(c, i))
        return remote(ref, ref, a_send.at[c], a_recv.at[c], (peers[i], s))

    def onward(c, i):
        ref = block(c, source_of(i), *passed(c, i))
        return remote(ref, ref, z_send.at[c], z_recv.at[c], (d, beside))

    def all_direct(c):
        ref = chunk(c).at[pl.ds(0, sum(span(c, i)[1] for i in range(n - 1))), :]
        return remote(ref, ref, a_send.at[c], a_recv.at[c], (peers[0], s))

    def all_onward(c):
        ref = chunk(c).at[pl.ds(0, sum(passed(c, i)[1] for i in relayed(c))), :]
        return remote(ref, ref, z_send.at[c], z_recv.at[c], (d, beside))

    def begin(c):
        local[c].wait()
        for i in range(n - 1):
            direct(c, i).start()

    def relay(c):
        if level[c]:
            all_direct(c).wait_recv()
            for i in relayed(c):
                onward(c, i).start()

    def finish(c):
        if level[c]:
            all_onward(c).wait_recv()
        else:
            all_direct(c).wait_recv()

    def swap(j):
        ref = wo_ref.at[j]
        at = lax.rem(j, groups)
        return remote(ref, ref, swap_send.at[at], swap_recv.at[at], (d, partner))

    pl.semaphore_wait(barrier, len(peers) + len(near))
    inputs[0].wait()
    field_up.start()
    field_down.start()
    for c in order:
        begin(c)

    unit = (lax.broadcasted_iota(jnp.int32, (channels, 128), 0)
            == lax.broadcasted_iota(jnp.int32, (channels, 128), 1)).astype(BF16)

    def turn(source, start, target):
        cells_ref[pl.ds(target, 512), :] = lax.dot_general(
            source[:, pl.ds(start, 512)], unit, (((0,), (0,)), ((), ())),
            preferred_element_type=F32)

    @pl.loop(0, cell_count // 512, unroll=2)
    def _(i):
        turn(field_ref, pl.multiple_of(i * 512, 512), pl.multiple_of(reach + i * 512, 512))

    for copy in inputs[1:]:
        copy.wait()
    pad = w_in_full.shape[0]
    w_in_full[pl.ds(pad - 32, 32), :] = jnp.zeros((32, width), BF16)
    w_in_full[pl.ds(0, channels), :] = w_in_ref[...]

    field_up.wait_recv()
    field_down.wait_recv()
    relay(order[0])

    @pl.loop(0, reach // 512)
    def _(i):
        turn(low_ref, pl.multiple_of(i * 512, 512), pl.multiple_of(i * 512, 512))
        turn(high_ref, pl.multiple_of(i * 512, 512),
             pl.multiple_of(reach + cell_count + i * 512, 512))

    def gather(first, last):
        @pl.loop(first, last)
        def _(b):
            base = pl.multiple_of(b * slots, slots)
            for j in range(slots):
                picked_ref[pl.ds(base + j, 1), :] = cells_ref[pl.ds(index_ref[b, j], 1), :]

    gather(0, blocks // 2)
    relay(order[1])
    gather(blocks // 2, blocks)

    own_base = margin + core * nodes
    own_edge = core * (nodes + margin)
    far_edge = (1 - core) * (nodes + margin)
    own_halo = core * (margin + 2 * nodes)
    far_halo = (1 - core) * (margin + 2 * nodes)
    far_base = margin + (1 - core) * nodes
    per_step = 8

    @pl.loop(0, blocks // per_step)
    def _(i):
        for j in range(per_step):
            b = i * per_step + j
            rows_b = picked_ref[pl.ds(pl.multiple_of(b * slots, slots), slots), :].astype(BF16)
            encoded = jnp.dot(weight_ref[b], rows_b, preferred_element_type=F32).astype(BF16)
            start = pl.multiple_of(b * per_block, per_block)
            enc_ref[pl.ds(pl.multiple_of(own_base + start, per_block), per_block), :] = encoded

    def enc_copy(target):
        edge = pl.multiple_of(margin + own_edge, margin)
        return remote(enc_ref.at[pl.ds(edge, margin), :],
                      enc_ref.at[pl.ds(pl.multiple_of(target, margin), margin), :],
                      enc_send.at[0], enc_recv.at[0], (d, outer))

    enc_copy(far_halo).start()

    def embed(start):
        embedded = jnp.dot(enc_ref[pl.ds(start, 128), :], w_in_full[...], preferred_element_type=F32)
        average = jnp.mean(embedded, axis=1, keepdims=True)
        centered = embedded - average
        spread = jnp.mean(centered * centered, axis=1, keepdims=True)
        normed_ref[pl.ds(start, 128), :] = (
            centered * lax.rsqrt(spread + 1e-05) * gain_ref[...]).astype(BF16)

    def norm_copy(i, start, size):
        ref = normed_ref.at[pl.ds(pl.multiple_of(start, margin), size), :]
        return remote(ref, ref, norm_send.at[i], norm_recv.at[i], (d, partner))

    for half_at in range(2):
        @pl.loop(0, margin // 128, unroll=2)
        def _(i):
            embed(pl.multiple_of(own_base + half_at * margin + i * 128, 128))

        norm_copy(half_at, own_base + half_at * margin, margin).start()

    relay(order[2])
    for half_at in range(2):
        latent_ref[pl.ds(half_at * margin, margin), :] = jnp.dot(
            enc_ref[pl.ds(pl.multiple_of(own_base + half_at * margin, margin), margin), :],
            w_in_full[...], preferred_element_type=F32).astype(BF16)

    def embed_halo():
        enc_copy(own_halo).wait_recv()

        @pl.loop(0, margin // 128, unroll=2)
        def _(i):
            embed(pl.multiple_of(own_halo + i * 128, 128))

        norm_copy(2, own_halo, margin).start()

    same_head = (lax.broadcasted_iota(jnp.int32, (gw, gw), 0) // head_size
                 == lax.broadcasted_iota(jnp.int32, (gw, gw), 1) // head_size).astype(BF16)

    def unit_heads(values):
        total = jnp.dot((values * values).astype(BF16), same_head, preferred_element_type=F32)
        return (values * lax.rsqrt(total * (1.0 / head_size) + 1e-06)).astype(BF16)

    scale = jnp.asarray(head_size ** -0.5, BF16)

    def project_part(start, size, c):
        if not isinstance(start, int):
            start = pl.multiple_of(start, margin)
        return jnp.dot(normed_ref[pl.ds(start, size), :], wq_ref[c], preferred_element_type=F32)

    def run(g, steps):
        def product(kind, start, size):
            return project_part(start, size, 3 * g + kind)

        later = product(*steps[0])
        for i, (kind, start, size) in enumerate(steps):
            part = later
            if i + 1 < len(steps):
                later = product(*steps[i + 1])
            if not isinstance(start, int):
                start = pl.multiple_of(start, margin)
            if kind == 0:
                q_ref[pl.ds(start - margin, size), :] = unit_heads(part) * scale
            elif kind == 1:
                k_ref[pl.ds(start, size), :] = unit_heads(part)
            else:
                vt_ref[:, pl.ds(start, size)] = part.astype(BF16).T

    inner = [(margin + i * nodes, nodes) for i in range(2)]
    edges = [(i * (margin + 2 * nodes), margin) for i in range(2)]

    head_of = lax.broadcasted_iota(jnp.int32, (nodes, gw), 1) // head_size

    def attend(t, slot):
        start = pl.multiple_of(t * nodes, nodes)
        asked = q_ref[pl.ds(start, nodes), :]
        seen = pl.ds(start, window)

        def score(h):
            picked = jnp.where(head_of == h, asked, jnp.zeros_like(asked))
            return lax.dot_general(k_ref[seen, :], picked, CONTRACT_LAST, preferred_element_type=F32)

        outs = []
        scores = score(0)
        for h in range(GROUP_HEADS):
            weights = jnp.exp(scores)
            if h + 1 < GROUP_HEADS:
                scores = score(h + 1)
            total = jnp.sum(weights, axis=0, keepdims=True)
            out = jnp.dot(vt_ref[pl.ds(h * head_size, head_size), seen], weights.astype(BF16),
                          preferred_element_type=F32)
            outs.append(out * (1.0 / total))
        att_ref[slot] = jnp.concatenate(outs, axis=0).astype(BF16).T

    def give(g, mine):
        at = core * groups + g if mine else (1 - core) * groups + g
        return remote(att_ref.at[parts + g], att_ref.at[at], give_send.at[g], give_recv.at[g],
                      (d, partner))

    def leave(j):
        columns = pl.ds(pl.multiple_of(j * gw, gw), gw)
        update_ref[:, columns] = sum(
            jnp.dot(att_ref[at], wo_ref[j, pl.ds(at * gw, gw), :], preferred_element_type=F32)
            for at in range(parts)).astype(BF16)

    finish(1)
    run(0, [(1, own_base, nodes)])
    for i in range(2):
        norm_copy(i, far_base + i * margin, margin).wait_recv()
    run(0, [(1, far_base, nodes)])
    finish(0)
    run(0, [(0, *at) for at in inner])
    relay(order[3])
    embed_halo()
    finish(2)
    relay(order[4])
    run(0, [(2, *at) for at in inner])
    norm_copy(2, far_halo, margin).wait_recv()
    run(0, [(1, *at) for at in edges] + [(2, *at) for at in edges])
    attend(1 - core, parts)
    give(0, True).start()
    relay(order[5])
    attend(core, core * groups)

    finish(4)
    finish(3)
    run(1, [(1, *at) for at in inner] + [(0, *at) for at in inner])
    relay(order[6])
    finish(5)
    run(1, [(1, *at) for at in edges] + [(2, *at) for at in inner + edges])
    attend(1 - core, parts + 1)
    give(1, True).start()
    finish(order[6])
    swap(groups * core).start()
    finish(order[7])
    swap(groups * core + 1).start()
    attend(core, core * groups + 1)

    for g in range(groups):
        give(g, False).wait_recv()
        swap(groups * (1 - core) + g).wait_recv()
    for j in range(parts):
        leave(j)
    for copy in (field_up, field_down, enc_copy(far_halo), norm_copy(0, own_base, margin),
                 norm_copy(1, own_base + margin, margin), norm_copy(2, own_halo, margin)):
        copy.wait_send()
    for g in range(groups):
        give(g, True).wait_send()
        swap(groups * core + g).wait_send()
    for c in order:
        all_direct(c).wait_send()
        if level[c]:
            all_onward(c).wait_send()


def deliver(latent_ref, update_ref, latent_hbm, update_hbm, sem):
    copies = [pltpu.make_async_copy(update_ref, update_hbm, sem.at[0]),
              pltpu.make_async_copy(latent_ref, latent_hbm, sem.at[1])]
    for copy in copies:
        copy.start()
    for copy in copies:
        copy.wait()


def shards(n, space, fields, cell_index, interp_weight, w_in, ln_gain, w_qkv, w_out):
    width = w_out.shape[1]
    blocks, per_block, _ = interp_weight.shape
    nodes = blocks * per_block
    channels, cells = fields.shape[1:]
    reach = cells // 4
    gw = width // HEADS * GROUP_HEADS
    parts = width // gw
    groups = parts // 2
    chunks = 3 * groups + parts // 2
    vmem = pl.BlockSpec(memory_space=pltpu.VMEM)
    hbm = pl.BlockSpec(memory_space=pl.ANY)
    dma = pltpu.SemaphoreType.DMA
    results = pl.pallas_call(
        functools.partial(kernel, n, space),
        out_shape=[pltpu.VMEM((nodes, width), BF16)] * 2,
        in_specs=[hbm] * 7,
        out_specs=[vmem] * 2,
        scratch_shapes=[
            pltpu.SMEM(cell_index.shape, jnp.int32),
            pltpu.VMEM((channels, cells), BF16),
            pltpu.VMEM(interp_weight.shape, BF16),
            pltpu.VMEM(w_in.shape, BF16),
            pltpu.VMEM((1, width), F32),
            pltpu.VMEM((channels, reach), BF16),
            pltpu.VMEM((channels, reach), BF16),
            pltpu.VMEM((cells + 2 * reach, 128), F32),
            pltpu.VMEM((blocks * 128, 128), F32),
            pltpu.VMEM((3 * nodes, 128), BF16),
            pltpu.VMEM((128, width), BF16),
            pltpu.VMEM((3 * nodes, width), BF16),
            pltpu.VMEM((3 * groups, width, gw), BF16),
            pltpu.VMEM((2 * nodes, gw), BF16),
            pltpu.VMEM((3 * nodes, gw), BF16),
            pltpu.VMEM((gw, 3 * nodes), BF16),
            pltpu.VMEM((parts + groups, nodes, gw), BF16),
            pltpu.VMEM((parts, width, gw), BF16),
            dma((5,)), dma((chunks,)),
            dma((2,)), dma((2,)), dma((1,)), dma((1,)), dma((3,)), dma((3,)),
            dma((chunks,)), dma((chunks,)), dma((chunks,)), dma((chunks,)),
            dma((groups,)), dma((groups,)), dma((groups,)), dma((groups,)),
        ],
        compiler_params=pltpu.CompilerParams(
            collective_id=0, has_side_effects=True, vmem_limit_bytes=40 * 2**20),
    )(*[pltpu.with_memory_space_constraint(array, pltpu.HBM) for array in (
        cell_index, fields[0], interp_weight, w_in, ln_gain[None], w_qkv, w_out)])

    latent, update = pl.pallas_call(
        deliver,
        out_shape=[jax.ShapeDtypeStruct((nodes, width), BF16)] * 2,
        in_specs=[vmem] * 2,
        out_specs=[hbm] * 2,
        scratch_shapes=[dma((2,))],
        compiler_params=pltpu.CompilerParams(vmem_limit_bytes=2**20),
    )(*[pltpu.with_memory_space_constraint(array, pltpu.VMEM) for array in results])
    return latent[None], update[None]


def solution(mesh):
    placed = (
        P("dp", None, "space"),
        P("space", None),
        P("space", None, None),
        P(),
        P(),
        P("dp", None),
        P("dp", None),
    )
    return jax.shard_map(
        functools.partial(shards, mesh.shape["dp"], mesh.shape["space"]),
        mesh=mesh,
        in_specs=placed,
        out_specs=(P("dp", "space", None), P("dp", "space", None)),
        check_vma=False,
    )
```

```python
import functools

import jax
import jax.numpy as jnp
from jax import lax
from jax.experimental import pallas as pl
from jax.experimental.pallas import tpu as pltpu
from jax.sharding import PartitionSpec as P

HEADS = 16
GROUP_HEADS = 4
F32, BF16 = jnp.float32, jnp.bfloat16
MESH = pl.DeviceIdType.MESH
SHARED = (2, 2, 2, 2, 2, 1, 2, 0)
CONTRACT_LAST = (((1,), (1,)), ((), ()))


def kernel(
    n, space, index_hbm, field_hbm, weight_hbm, w_in_hbm, gain_hbm, w_qkv_hbm, w_out_hbm,
    latent_ref, update_ref,
    index_ref, field_ref, weight_ref, w_in_ref, gain_ref,
    low_ref, high_ref, cells_ref, picked_ref, enc_ref, w_in_full, normed_ref, wq_ref,
    q_ref, k_ref, vt_ref, att_ref, wo_ref, weight_of, total_ref,
    in_sem, local_sem, field_send, field_recv, enc_send, enc_recv, norm_send, norm_recv,
    a_send, a_recv, z_send, z_recv, swap_send, swap_recv, give_send, give_recv,
):
    d, s = lax.axis_index("dp"), lax.axis_index("space")
    up, down = lax.rem(s + 1, space), lax.rem(s + space - 1, space)
    core = lax.rem(s, 2)
    partner = s + 1 - 2 * core
    outer = lax.rem(s + space - 1 + 2 * core, space)
    layer = lax.rem(s // 2, 2)
    beside = s + 2 - 4 * layer
    share = n == 4 and space % 4 == 0
    channels, cell_count = field_ref.shape
    reach = low_ref.shape[1]
    rows, width = w_out_hbm.shape
    gw = q_ref.shape[1]
    parts = width // gw
    groups = parts // 2
    chunks = 3 * groups + parts // 2
    head_size = gw // GROUP_HEADS
    nodes = latent_ref.shape[0]
    margin = nodes // 2
    window = nodes + 2 * margin
    blocks, per_block, slots = weight_ref.shape
    if n == 4:
        peers = [d + 1 - 2 * lax.rem(d, 2), lax.rem(d + 2, 4), 3 - d]
    else:
        peers = [lax.rem(d + i, n) for i in range(1, n)]

    def source_of(i):
        return peers[i] if n == 4 else peers[n - 2 - i]

    barrier = pltpu.get_barrier_semaphore()
    for peer in peers:
        pl.semaphore_signal(barrier, inc=1, device_id=(peer, s), device_id_type=MESH)
    near = (up, down, beside) if share else (up, down)
    for peer in near:
        pl.semaphore_signal(barrier, inc=1, device_id=(d, peer), device_id_type=MESH)

    inputs = [
        pltpu.make_async_copy(source, target, in_sem.at[i])
        for i, (source, target) in enumerate((
            (field_hbm, field_ref), (index_hbm, index_ref), (weight_hbm, weight_ref),
            (w_in_hbm, w_in_ref), (gain_hbm, gain_ref)))
    ]
    for copy in inputs:
        copy.start()

    def chunk(c):
        return wq_ref.at[c] if c < 3 * groups else wo_ref.at[groups * core + c - 3 * groups]

    own = pl.ds(pl.multiple_of(d * rows, rows), rows)
    order = [3 * g + t for g in range(groups) for t in (1, 0, 2)]
    order += range(3 * groups, chunks)
    local = {}
    for c in order:
        if c < 3 * groups:
            column = c % 3 * width + (core * groups + c // 3) * gw
            source = w_qkv_hbm.at[:, pl.ds(pl.multiple_of(column, gw), gw)]
        else:
            column = (core * groups + c - 3 * groups) * gw
            source = w_out_hbm.at[:, pl.ds(pl.multiple_of(column, gw), gw)]
        local[c] = pltpu.make_async_copy(source, chunk(c).at[own, :], local_sem.at[c])
        local[c].start()

    def remote(src, dst, send, recv, device):
        return pltpu.make_async_remote_copy(
            src_ref=src, dst_ref=dst, send_sem=send, recv_sem=recv,
            device_id=device, device_id_type=MESH)

    field_up = remote(field_ref.at[:, pl.ds(cell_count - reach, reach)], low_ref,
                      field_send.at[0], field_recv.at[0], (d, up))
    field_down = remote(field_ref.at[:, pl.ds(0, reach)], high_ref,
                        field_send.at[1], field_recv.at[1], (d, down))

    whole = rows * 11 // 256 * 16
    half = rows // 2

    level = {c: SHARED[at] if share else 0 for at, c in enumerate(order)}

    def span(c, i):
        if i == 2 and level[c]:
            return layer * half, half
        if level[c] == 2:
            return layer * (rows - whole), whole
        return 0, rows

    def passed(c, i):
        if i == 2 and level[c]:
            return layer * half, half
        return layer * whole, rows - whole

    def relayed(c):
        return [(), (2,), (0, 1, 2)][level[c]]

    def block(c, owner, lo, size):
        return chunk(c).at[pl.ds(pl.multiple_of(owner * rows + lo, 16), size), :]

    def direct(c, i):
        ref = block(c, d, *span(c, i))
        return remote(ref, ref, a_send.at[c], a_recv.at[c], (peers[i], s))

    def onward(c, i):
        ref = block(c, source_of(i), *passed(c, i))
        return remote(ref, ref, z_send.at[c], z_recv.at[c], (d, beside))

    def all_direct(c):
        ref = chunk(c).at[pl.ds(0, sum(span(c, i)[1] for i in range(n - 1))), :]
        return remote(ref, ref, a_send.at[c], a_recv.at[c], (peers[0], s))

    def all_onward(c):
        ref = chunk(c).at[pl.ds(0, sum(passed(c, i)[1] for i in relayed(c))), :]
        return remote(ref, ref, z_send.at[c], z_recv.at[c], (d, beside))

    def begin(c):
        local[c].wait()
        for i in range(n - 1):
            direct(c, i).start()

    def relay(c):
        if level[c]:
            all_direct(c).wait_recv()
            for i in relayed(c):
                onward(c, i).start()

    def finish(c):
        if level[c]:
            all_onward(c).wait_recv()
        else:
            all_direct(c).wait_recv()

    def swap(j):
        ref = wo_ref.at[j]
        at = lax.rem(j, groups)
        return remote(ref, ref, swap_send.at[at], swap_recv.at[at], (d, partner))

    pl.semaphore_wait(barrier, len(peers) + len(near))
    inputs[0].wait()
    field_up.start()
    field_down.start()
    for c in order:
        begin(c)

    unit = (lax.broadcasted_iota(jnp.int32, (channels, 128), 0)
            == lax.broadcasted_iota(jnp.int32, (channels, 128), 1)).astype(BF16)

    def turn(source, start, target):
        cells_ref[pl.ds(target, 512), :] = lax.dot_general(
            source[:, pl.ds(start, 512)], unit, (((0,), (0,)), ((), ())),
            preferred_element_type=F32)

    @pl.loop(0, cell_count // 512, unroll=2)
    def _(i):
        turn(field_ref, pl.multiple_of(i * 512, 512), pl.multiple_of(reach + i * 512, 512))

    for copy in inputs[1:]:
        copy.wait()
    pad = w_in_full.shape[0]
    w_in_full[pl.ds(pad - 32, 32), :] = jnp.zeros((32, width), BF16)
    w_in_full[pl.ds(0, channels), :] = w_in_ref[...]

    field_up.wait_recv()
    field_down.wait_recv()
    relay(order[0])

    @pl.loop(0, reach // 512)
    def _(i):
        turn(low_ref, pl.multiple_of(i * 512, 512), pl.multiple_of(i * 512, 512))
        turn(high_ref, pl.multiple_of(i * 512, 512),
             pl.multiple_of(reach + cell_count + i * 512, 512))

    def gather(first, last):
        @pl.loop(first, last)
        def _(b):
            base = pl.multiple_of(b * slots, slots)
            for j in range(slots):
                picked_ref[pl.ds(base + j, 1), :] = cells_ref[pl.ds(index_ref[b, j], 1), :]

    gather(0, blocks // 2)
    relay(order[1])
    gather(blocks // 2, blocks)

    own_base = margin + core * nodes
    own_edge = core * (nodes + margin)
    far_edge = (1 - core) * (nodes + margin)
    own_halo = core * (margin + 2 * nodes)
    far_halo = (1 - core) * (margin + 2 * nodes)
    far_base = margin + (1 - core) * nodes
    per_step = 8

    @pl.loop(0, blocks // per_step)
    def _(i):
        for j in range(per_step):
            b = i * per_step + j
            rows_b = picked_ref[pl.ds(pl.multiple_of(b * slots, slots), slots), :].astype(BF16)
            encoded = jnp.dot(weight_ref[b], rows_b, preferred_element_type=F32).astype(BF16)
            start = pl.multiple_of(b * per_block, per_block)
            enc_ref[pl.ds(pl.multiple_of(own_base + start, per_block), per_block), :] = encoded

    def enc_copy(target):
        edge = pl.multiple_of(margin + own_edge, margin)
        return remote(enc_ref.at[pl.ds(edge, margin), :],
                      enc_ref.at[pl.ds(pl.multiple_of(target, margin), margin), :],
                      enc_send.at[0], enc_recv.at[0], (d, outer))

    enc_copy(far_halo).start()

    def embed(start):
        embedded = jnp.dot(enc_ref[pl.ds(start, 128), :], w_in_full[...], preferred_element_type=F32)
        average = jnp.mean(embedded, axis=1, keepdims=True)
        centered = embedded - average
        spread = jnp.mean(centered * centered, axis=1, keepdims=True)
        normed_ref[pl.ds(start, 128), :] = (
            centered * lax.rsqrt(spread + 1e-05) * gain_ref[...]).astype(BF16)

    def norm_copy(i, start, size):
        ref = normed_ref.at[pl.ds(pl.multiple_of(start, margin), size), :]
        return remote(ref, ref, norm_send.at[i], norm_recv.at[i], (d, partner))

    for half_at in range(2):
        @pl.loop(0, margin // 128, unroll=2)
        def _(i):
            embed(pl.multiple_of(own_base + half_at * margin + i * 128, 128))

        norm_copy(half_at, own_base + half_at * margin, margin).start()

    relay(order[2])
    for half_at in range(2):
        latent_ref[pl.ds(half_at * margin, margin), :] = jnp.dot(
            enc_ref[pl.ds(pl.multiple_of(own_base + half_at * margin, margin), margin), :],
            w_in_full[...], preferred_element_type=F32).astype(BF16)

    def embed_halo():
        enc_copy(own_halo).wait_recv()

        @pl.loop(0, margin // 128, unroll=2)
        def _(i):
            embed(pl.multiple_of(own_halo + i * 128, 128))

        norm_copy(2, own_halo, margin).start()

    same_head = (lax.broadcasted_iota(jnp.int32, (gw, gw), 0) // head_size
                 == lax.broadcasted_iota(jnp.int32, (gw, gw), 1) // head_size).astype(BF16)

    def unit_heads(values):
        total = jnp.dot((values * values).astype(BF16), same_head, preferred_element_type=F32)
        return (values * lax.rsqrt(total * (1.0 / head_size) + 1e-06)).astype(BF16)

    scale = jnp.asarray(head_size ** -0.5, BF16)

    def project_part(start, size, c):
        if not isinstance(start, int):
            start = pl.multiple_of(start, margin)
        return jnp.dot(normed_ref[pl.ds(start, size), :], wq_ref[c], preferred_element_type=F32)

    def run(g, steps):
        def product(kind, start, size):
            return project_part(start, size, 3 * g + kind)

        later = product(*steps[0])
        for i, (kind, start, size) in enumerate(steps):
            part = later
            if i + 1 < len(steps):
                later = product(*steps[i + 1])
            if not isinstance(start, int):
                start = pl.multiple_of(start, margin)
            if kind == 0:
                q_ref[pl.ds(start - margin, size), :] = unit_heads(part) * scale
            elif kind == 1:
                k_ref[pl.ds(start, size), :] = unit_heads(part)
            else:
                vt_ref[:, pl.ds(start, size)] = part.astype(BF16).T

    inner = [(margin + i * nodes, nodes) for i in range(2)]
    edges = [(i * (margin + 2 * nodes), margin) for i in range(2)]

    head_of = lax.broadcasted_iota(jnp.int32, (nodes, gw), 1) // head_size

    def weigh(t, h):
        start = pl.multiple_of(t * nodes, nodes)
        asked = q_ref[pl.ds(start, nodes), :]
        picked = jnp.where(head_of == h, asked, jnp.zeros_like(asked))
        return jnp.exp(lax.dot_general(
            k_ref[pl.ds(start, window), :], picked, CONTRACT_LAST, preferred_element_type=F32))

    def mix(t, h, weights, total):
        seen = pl.ds(pl.multiple_of(t * nodes, nodes), window)
        return jnp.dot(vt_ref[pl.ds(h * head_size, head_size), seen], weights,
                       preferred_element_type=F32) * (1.0 / total)

    def settle(slot, h, outs):
        att_ref[slot, :, h * head_size:(h + len(outs)) * head_size] = (
            jnp.concatenate(outs, axis=0).astype(BF16).T)

    def attend(t, slot, heads=range(GROUP_HEADS)):
        outs = []
        weights = weigh(t, heads[0])
        for h in heads:
            later = weigh(t, h + 1) if h + 1 < heads.stop else None
            total = jnp.sum(weights, axis=0, keepdims=True)
            outs.append(mix(t, h, weights.astype(BF16), total))
            weights = later
        settle(slot, heads[0], outs)

    def prepare(t):
        for h in range(GROUP_HEADS):
            weights = weigh(t, h)
            total_ref[pl.ds(h, 1), :] = jnp.sum(weights, axis=0, keepdims=True)
            weight_of[h] = weights.astype(BF16)

    def conclude(t, slot):
        settle(slot, 0, [mix(t, h, weight_of[h], total_ref[pl.ds(h, 1), :])
                         for h in range(GROUP_HEADS)])

    def give(g, mine):
        at = core * groups + g if mine else (1 - core) * groups + g
        return remote(att_ref.at[parts + g], att_ref.at[at], give_send.at[g], give_recv.at[g],
                      (d, partner))

    def leave(j):
        columns = pl.ds(pl.multiple_of(j * gw, gw), gw)
        update_ref[:, columns] = sum(
            jnp.dot(att_ref[at], wo_ref[j, pl.ds(at * gw, gw), :], preferred_element_type=F32)
            for at in range(parts)).astype(BF16)

    finish(1)
    run(0, [(1, own_base, nodes)])
    for i in range(2):
        norm_copy(i, far_base + i * margin, margin).wait_recv()
    run(0, [(1, far_base, nodes)])
    finish(0)
    run(0, [(0, *at) for at in inner])
    relay(order[3])
    embed_halo()
    norm_copy(2, far_halo, margin).wait_recv()
    run(0, [(1, *at) for at in edges])
    relay(order[4])
    prepare(1 - core)
    finish(2)
    run(0, [(2, *at) for at in inner + edges])
    conclude(1 - core, parts)
    give(0, True).start()
    relay(order[5])
    attend(core, core * groups)

    finish(4)
    finish(3)
    run(1, [(1, *at) for at in inner] + [(0, *at) for at in inner])
    relay(order[6])
    finish(5)
    run(1, [(1, *at) for at in edges] + [(2, *at) for at in inner + edges])
    attend(1 - core, parts + 1)
    give(1, True).start()
    finish(order[6])
    swap(groups * core).start()
    finish(order[7])
    swap(groups * core + 1).start()
    attend(core, core * groups + 1)

    for g in range(groups):
        give(g, False).wait_recv()
        swap(groups * (1 - core) + g).wait_recv()
    for j in range(parts):
        leave(j)
    for copy in (field_up, field_down, enc_copy(far_halo), norm_copy(0, own_base, margin),
                 norm_copy(1, own_base + margin, margin), norm_copy(2, own_halo, margin)):
        copy.wait_send()
    for g in range(groups):
        give(g, True).wait_send()
        swap(groups * core + g).wait_send()
    for c in order:
        all_direct(c).wait_send()
        if level[c]:
            all_onward(c).wait_send()


def deliver(latent_ref, update_ref, latent_hbm, update_hbm, sem):
    copies = [pltpu.make_async_copy(update_ref, update_hbm, sem.at[0]),
              pltpu.make_async_copy(latent_ref, latent_hbm, sem.at[1])]
    for copy in copies:
        copy.start()
    for copy in copies:
        copy.wait()


def shards(n, space, fields, cell_index, interp_weight, w_in, ln_gain, w_qkv, w_out):
    width = w_out.shape[1]
    blocks, per_block, _ = interp_weight.shape
    nodes = blocks * per_block
    channels, cells = fields.shape[1:]
    reach = cells // 4
    gw = width // HEADS * GROUP_HEADS
    parts = width // gw
    groups = parts // 2
    chunks = 3 * groups + parts // 2
    vmem = pl.BlockSpec(memory_space=pltpu.VMEM)
    hbm = pl.BlockSpec(memory_space=pl.ANY)
    dma = pltpu.SemaphoreType.DMA
    results = pl.pallas_call(
        functools.partial(kernel, n, space),
        out_shape=[pltpu.VMEM((nodes, width), BF16)] * 2,
        in_specs=[hbm] * 7,
        out_specs=[vmem] * 2,
        scratch_shapes=[
            pltpu.SMEM(cell_index.shape, jnp.int32),
            pltpu.VMEM((channels, cells), BF16),
            pltpu.VMEM(interp_weight.shape, BF16),
            pltpu.VMEM(w_in.shape, BF16),
            pltpu.VMEM((1, width), F32),
            pltpu.VMEM((channels, reach), BF16),
            pltpu.VMEM((channels, reach), BF16),
            pltpu.VMEM((cells + 2 * reach, 128), F32),
            pltpu.VMEM((blocks * 128, 128), F32),
            pltpu.VMEM((3 * nodes, 128), BF16),
            pltpu.VMEM((128, width), BF16),
            pltpu.VMEM((3 * nodes, width), BF16),
            pltpu.VMEM((3 * groups, width, gw), BF16),
            pltpu.VMEM((2 * nodes, gw), BF16),
            pltpu.VMEM((3 * nodes, gw), BF16),
            pltpu.VMEM((gw, 3 * nodes), BF16),
            pltpu.VMEM((parts + groups, nodes, gw), BF16),
            pltpu.VMEM((parts, width, gw), BF16),
            pltpu.VMEM((GROUP_HEADS, 2 * nodes, nodes), BF16),
            pltpu.VMEM((8, nodes), F32),
            dma((5,)), dma((chunks,)),
            dma((2,)), dma((2,)), dma((1,)), dma((1,)), dma((3,)), dma((3,)),
            dma((chunks,)), dma((chunks,)), dma((chunks,)), dma((chunks,)),
            dma((groups,)), dma((groups,)), dma((groups,)), dma((groups,)),
        ],
        compiler_params=pltpu.CompilerParams(
            collective_id=0, has_side_effects=True, vmem_limit_bytes=40 * 2**20),
    )(*[pltpu.with_memory_space_constraint(array, pltpu.HBM) for array in (
        cell_index, fields[0], interp_weight, w_in, ln_gain[None], w_qkv, w_out)])

    latent, update = pl.pallas_call(
        deliver,
        out_shape=[jax.ShapeDtypeStruct((nodes, width), BF16)] * 2,
        in_specs=[vmem] * 2,
        out_specs=[hbm] * 2,
        scratch_shapes=[dma((2,))],
        compiler_params=pltpu.CompilerParams(vmem_limit_bytes=2**20),
    )(*[pltpu.with_memory_space_constraint(array, pltpu.VMEM) for array in results])
    return latent[None], update[None]


def solution(mesh):
    placed = (
        P("dp", None, "space"),
        P("space", None),
        P("space", None, None),
        P(),
        P(),
        P("dp", None),
        P("dp", None),
    )
    return jax.shard_map(
        functools.partial(shards, mesh.shape["dp"], mesh.shape["space"]),
        mesh=mesh,
        in_specs=placed,
        out_specs=(P("dp", "space", None), P("dp", "space", None)),
        check_vma=False,
    )
```
